256 devices in a mesh: pair: 128 (over x_hi, z, y, core), ao: 2 (over x_lo).
Axes of the slice: x: 4 (x_hi: 2, x_lo: 2; x = x_hi * 2 + x_lo), y: 4, z: 8, core: 2. Of those that a mesh axis runs over, the one named last changes fastest.
Arguments:
- gamma: bfloat16 [128, 1792, 1792], P('pair', 'ao'), may hold values from -6 to 6
- c_vir: bfloat16 [1024, 1792], replicated, may hold values from -0.125 to 0.125
- c_occ: bfloat16 [1024, 256], replicated, may hold values from -1.796875 to 1.796875
- pair_list: int32 [128, 2], replicated, may hold values from 0 to 255
- shell_order: int32 [128], replicated, may hold values from 0 to 127, each once
Outputs:
- ao_density: bfloat16 [1024, 1024], P('ao', 'pair')
The draws below stay inside these ranges and needn't reach their ends.
Inputs may be any that keep to these rules, and one draw needn't show every extreme that they name: shell_order holds each of 0 to 127 once.
All inputs are finite; a program needn't handle non-finite values.
Results may differ from the reference program's by a relative error of at most 0.0049.
Values sent between devices are 32-bit elements; how exact they have to be, the bound alone decides.
A program may use at most 64 MiB of HBM per device.

```python
import jax
import jax.numpy as jnp
from jax import lax

NBF = 1024
V = 1792
OCC = 256
SB = 8
PAIRS = 128
SHELLS = 128


def touch_ends(drawn, key, least, high):
    shape = drawn.shape
    spot = [jax.random.randint(jax.random.fold_in(key, axis), (), 0, shape[axis]) for axis in range(len(shape))]
    drawn = drawn.at[tuple(spot)].set(least)
    longest = shape.index(max(shape))
    spot[longest] = (spot[longest] + 1) % shape[longest]
    return drawn.at[tuple(spot)].set(high)


def level_of(key, extent, shards, smallest, high):
    factor_of, own = 1.0, jax.random.fold_in(key, 6)
    for position, shards_of in shards:
        heights = jnp.exp(jax.random.uniform(jax.random.fold_in(own, position), (shards_of,), jnp.float32, smallest / len(shards), high / len(shards)))
        factor_of = factor_of * jnp.repeat(heights, extent[position] // shards_of).reshape([-1 if axis == position else 1 for axis in range(len(extent))])
    return factor_of


def normal_values(rng, dims, scale, limit, cuts=(), kind=jnp.bfloat16):
    drawn = scale * jax.random.normal(rng, dims, jnp.float32)
    if cuts:
        drawn = drawn * level_of(rng, dims, cuts, -0.22, 0.18)
    return jnp.clip(drawn, -limit, limit).astype(kind)


def setup_inputs(seed: int = 0) -> dict:
    splits = jax.random.split(jax.random.key(seed), 6)
    return {
        "gamma": normal_values(splits[0], (PAIRS, V, V), 1.0, 6.0, ((0, 128), (1, 2))),
        "c_vir": normal_values(splits[1], (NBF, V), V ** -0.5, 0.125),
        "c_occ": normal_values(splits[2], (NBF, OCC), 0.3, 1.796875),
        "pair_list": touch_ends(jax.random.randint(splits[3], (PAIRS, 2), 0, OCC), jax.random.fold_in(splits[3], 1), 0, OCC - 1).astype(jnp.int32),
        "shell_order": jax.random.permutation(splits[4], SHELLS).astype(jnp.int32),
    }


def reference(gamma, c_vir, c_occ, pair_list, shell_order):
    offsets = jnp.arange(SB, dtype=jnp.int32)
    row_index = (shell_order[:, None].astype(jnp.int32) * SB + offsets[None, :]).reshape(-1)
    vir_sorted = c_vir[row_index]
    occ_sorted = c_occ[row_index]

    def add_pair(total, inputs):
        amplitude, pair_ids = inputs
        half_block = lax.dot_general(amplitude, c_vir, (((1,), (1,)), ((), ())),
                                     preferred_element_type=jnp.float32).astype(jnp.bfloat16)
        ao_block = lax.dot_general(half_block, vir_sorted, (((0,), (1,)), ((), ())),
                                   preferred_element_type=jnp.float32)
        left_weight = occ_sorted[:, pair_ids[0]].astype(jnp.float32)
        right_weight = c_occ[:, pair_ids[1]].astype(jnp.float32)
        return total + right_weight[:, None] * ao_block * left_weight[None, :], None

    total, _ = lax.scan(add_pair, jnp.zeros((NBF, NBF), jnp.float32), (gamma, pair_list))
    return total.astype(jnp.bfloat16)
```

```python
import jax
import jax.numpy as jnp
from jax import lax
from jax.experimental import pallas as pl
from jax.experimental.pallas import tpu as pltpu
from jax.sharding import PartitionSpec as P

MESH = pl.DeviceIdType.MESH
SB = 8
XS, YS, ZS = 4, 4, 8
NCH = 4
LANES = 128


def kernel(gamma, c_vir, c_occ, pairs, shells, out, g, cv, co, pair_s, shell_s,
           lw, rw, half, block, s_buf, r_d, r_1, r_2, r_3, c_buf, r_z,
           in_sem, d_send, d_recv, send_1, recv_1, send_2, recv_2, send_3, recv_3, send_z, recv_z):
    local, vir = g.shape
    basis = cv.shape[0]
    pair = lax.axis_index("pair")
    xlo = lax.axis_index("ao")
    core = pair % 2
    y = (pair // 2) % YS
    z = (pair // (2 * YS)) % ZS
    xhi = pair // (2 * YS * ZS)
    yhi, ylo = y // 2, y % 2

    def device(xh, xl, yy, zz, cc):
        return (((xh * ZS + zz) * YS + yy) * 2 + cc, xl)

    def relative(hi, lo, a, b, c):
        own = (hi + lo * (1 - c)) % 2
        low = (lo + b) % 2
        return ((own + a) % 2 + low * (1 - c)) % 2, low

    def x_peer(a, b):
        hi, lo = relative(xhi, xlo, a, b, core)
        return device(hi, lo, y, z, core)

    def y_peer(a, b):
        hi, lo = relative(yhi, ylo, a, b, core)
        return device(xhi, xlo, hi * 2 + lo, z, core)

    def z_peer(dz):
        return device(xhi, xlo, y, (z + dz) % ZS, core)

    twin = device(xhi, xlo, y, z, 1 - core)
    x_first = device((xhi + core) % 2, 1 - xlo, y, z, core)
    y_first = device(xhi, xlo, ((yhi + core) % 2) * 2 + (1 - ylo), z, core)
    x_second = x_peer(0, 1)
    y_second = y_peer(0, 1)

    own_half = xlo * (basis // 2)
    other_half = (1 - xlo) * (basis // 2)

    def row_starts(j):
        return (pl.multiple_of(own_half + j * LANES, LANES), pl.multiple_of(other_half + j * LANES, LANES))

    copies = {}

    def load(name, src, dst, k):
        copies[name] = pltpu.make_async_copy(src, dst, in_sem.at[k])
        copies[name].start()

    load("shell", shells, shell_s, 0)
    load("pair", pairs, pair_s, 1)
    count = 2
    mid = local // 2
    for t, start in enumerate(row_starts(0)):
        load(("cv", 0, t), c_vir.at[pl.ds(start, LANES)], cv.at[pl.ds(start, LANES)], count)
        count += 1
    for t in range(2):
        load(("g", t), gamma.at[0, pl.ds(t * mid, mid)], g.at[pl.ds(t * mid, mid)], count)
        count += 1
    load("co", c_occ, co, count)
    count += 1
    for j in range(1, NCH):
        for t, start in enumerate(row_starts(j)):
            load(("cv", j, t), c_vir.at[pl.ds(start, LANES)], cv.at[pl.ds(start, LANES)], count)
            count += 1

    barrier = pltpu.get_barrier_semaphore()
    peers = [twin]
    peers += [x_peer(a, b) for a, b in ((0, 1), (1, 0), (1, 1))]
    peers += [y_peer(a, b) for a, b in ((0, 1), (1, 0), (1, 1))]
    peers += [z_peer(dz) for dz in range(1, ZS)]
    for peer in peers:
        pl.semaphore_signal(barrier, inc=1, device_id=peer, device_id_type=MESH)

    copies["shell"].wait()
    bits = [(a, b) for a in range(2) for b in range(2)]
    z_part = [((z + dz) % ZS) * (2 * YS) for dz in range(ZS)]
    x_part, y_part = {}, {}
    for d in range(2):
        cc = (core + d) % 2
        for a, b in bits:
            hi, lo = relative(xhi, xlo, a, b, cc)
            x_part[d, a, b] = hi * (2 * YS * ZS) + cc
            hi, lo = relative(yhi, ylo, a, b, cc)
            y_part[d, a, b] = (hi * 2 + lo) * 2

    def weights():
        copies["pair"].wait()
        copies["co"].wait()
        left = pair_s[0, pair]
        right = pair_s[1, pair]
        occ = co.shape[1]
        pick = jnp.where(lax.broadcasted_iota(jnp.int32, (occ, LANES), 0) == left, 1.0, 0.0).astype(jnp.bfloat16)
        lw[...] = jnp.dot(co[...], pick, preferred_element_type=jnp.float32).reshape(lw.shape)
        pick = jnp.where(lax.broadcasted_iota(jnp.int32, (16, occ), 1) == right, 1.0, 0.0).astype(jnp.bfloat16)
        rw[...] = lax.dot_general(pick, co[...], (((1,), (1,)), ((), ())), preferred_element_type=jnp.float32)[:8]

    def compute_half(j):
        starts = row_starts(j)
        rhs = jnp.concatenate([cv[pl.ds(start, LANES), :] for start in starts], axis=0)
        for t in range(2):
            if j == 0:
                copies["g", t].wait()
            half[pl.ds(t * mid, mid), :] = lax.dot_general(
                g[pl.ds(t * mid, mid), :], rhs, (((1,), (1,)), ((), ())), preferred_element_type=jnp.float32
            ).astype(jnp.bfloat16)

    def compute_block(j):
        column = pl.multiple_of(xlo * local, LANES)
        tall = basis // 2
        for t in range(2):
            block[pl.ds(t * tall // SB, tall // SB)] = jnp.dot(
                cv[pl.ds(t * tall, tall), pl.ds(column, local)], half[...], preferred_element_type=jnp.float32
            ).reshape(tall // SB, SB, 2 * LANES)

    def remote(src, dst, send, recv, peer):
        return pltpu.make_async_remote_copy(
            src_ref=src, dst_ref=dst, send_sem=send, recv_sem=recv, device_id=peer, device_id_type=MESH)

    def copy_d(j):
        return remote(s_buf.at[j, 1], r_d.at[j], d_send.at[j], d_recv.at[j], twin)

    def copy_1(j, part):
        return remote(s_buf.at[j, 0, part, pl.ds(32, 32)], r_1.at[j, part], send_1.at[j, part], recv_1.at[j, part],
                      (x_first, y_first)[part])

    def copy_2(j, part):
        return remote(s_buf.at[j, 0, part, pl.ds(16, 16)], r_2.at[j, part], send_2.at[j, part], recv_2.at[j, part],
                      (x_second, y_second)[part])

    def copy_3(j, part, t):
        a, b = bits[t]
        return remote(s_buf.at[j, 0, part, pl.ds(t * 4, 4)], r_3.at[j, part, t - 1], send_3.at[j, part, t - 1],
                      recv_3.at[j, part, t - 1], (y_peer if part == 0 else x_peer)(a, b))

    def copy_z(j, dz):
        return remote(c_buf.at[j, dz], r_z.at[j, dz - 1], send_z.at[j, dz - 1], recv_z.at[j, dz - 1], z_peer(dz))

    def weigh(j):
        right = [rw[:, pl.ds(start, LANES)] for start in row_starts(j)]
        for d in (1, 0):
            for part in range(2):
                for u in range(4):
                    for v in range(4):
                        xb, yb = (bits[u], bits[v]) if part == 0 else (bits[v], bits[u])
                        xy = x_part[(d,) + xb] + y_part[(d,) + yb]
                        b = xb[1]
                        for w in range(4):
                            shell = shell_s[xy + z_part[part * 4 + w]]
                            tile = block[shell, :, b * LANES : (b + 1) * LANES] * right[b]
                            s_buf[j, d, part, (u * 4 + v) * 4 + w] = tile * lw[shell]
            if d == 1:
                copy_d(j).start()

    def stage_c(j):
        if j == 0:
            for t in range(2):
                copies["cv", 0, t].wait()
        compute_half(j)
        if j == 0:
            for k in range(1, NCH):
                for t in range(2):
                    copies["cv", k, t].wait()
            weights()
        compute_block(j)
        if j == 0:
            pl.semaphore_wait(barrier, len(peers))
        weigh(j)

    def stage_e(j):
        copy_d(j).wait_recv()
        for part in range(2):
            s_buf[j, 0, part, pl.ds(32, 32)] = s_buf[j, 0, part, pl.ds(32, 32)] + r_d[j, part, pl.ds(32, 32)]
            copy_1(j, part).start()
        for part in range(2):
            s_buf[j, 0, part, pl.ds(0, 32)] = s_buf[j, 0, part, pl.ds(0, 32)] + r_d[j, part, pl.ds(0, 32)]

    def stage_f(j):
        for part in range(2):
            copy_1(j, part).wait_recv()
            s_buf[j, 0, part, pl.ds(16, 16)] = s_buf[j, 0, part, pl.ds(16, 16)] + r_1[j, part, pl.ds(0, 16)]
            copy_2(j, part).start()
            s_buf[j, 0, part, pl.ds(0, 16)] = s_buf[j, 0, part, pl.ds(0, 16)] + r_1[j, part, pl.ds(16, 16)]

    def stage_g(j):
        for part in range(2):
            copy_2(j, part).wait_recv()
            s_buf[j, 0, part, pl.ds(0, 16)] = s_buf[j, 0, part, pl.ds(0, 16)] + r_2[j, part]
            for t in (3, 2, 1):
                copy_3(j, part, t).start()

    def stage_h(j):
        for part in range(2):
            total = s_buf[j, 0, part, pl.ds(0, 4)]
            for t in (1, 2, 3):
                copy_3(j, part, t).wait_recv()
                total = total + r_3[j, part, t - 1]
            c_buf[j, pl.ds(part * 4, 4)] = total
        for dz in (4, 3, 5, 2, 6, 1, 7):
            copy_z(j, dz).start()

    def stage_i(j):
        total = c_buf[j, 0]
        for dz in range(1, ZS):
            copy_z(j, dz).wait_recv()
            total = total + r_z[j, dz - 1]
        out[:, j * LANES : (j + 1) * LANES] = total

    order = (stage_c, 0), (stage_c, 1), (stage_e, 0), (stage_c, 2), (stage_e, 1), (stage_c, 3), (stage_e, 2), (stage_f, 0)
    order += (stage_e, 3), (stage_f, 1), (stage_g, 0), (stage_f, 2), (stage_g, 1), (stage_f, 3), (stage_h, 0), (stage_g, 2)
    order += (stage_h, 1), (stage_g, 3), (stage_h, 2), (stage_i, 0), (stage_h, 3), (stage_i, 1), (stage_i, 2), (stage_i, 3)
    for stage, j in order:
        stage(j)
    for j in range(NCH):
        copy_d(j).wait_send()
        for part in range(2):
            copy_1(j, part).wait_send()
            copy_2(j, part).wait_send()
            for t in (1, 2, 3):
                copy_3(j, part, t).wait_send()
        for dz in range(1, ZS):
            copy_z(j, dz).wait_send()


def shards(gamma, c_vir, c_occ, pair_list, shell_order):
    local, vir = gamma.shape[1:]
    basis = c_vir.shape[0]
    f32, bf16 = jnp.float32, jnp.bfloat16
    dma = pltpu.SemaphoreType.DMA
    tile = (SB, LANES)
    summed = pl.pallas_call(
        kernel,
        out_shape=jax.ShapeDtypeStruct((SB, basis // 2), f32),
        in_specs=[pl.BlockSpec(memory_space=pl.ANY)] * 5,
        out_specs=pl.BlockSpec(memory_space=pltpu.VMEM),
        scratch_shapes=[
            pltpu.VMEM((local, vir), bf16),
            pltpu.VMEM((basis, vir), bf16),
            pltpu.VMEM(c_occ.shape, bf16),
            pltpu.SMEM((2, pair_list.shape[0]), jnp.int32),
            pltpu.SMEM(shell_order.shape, jnp.int32),
            pltpu.VMEM((basis // SB, SB, LANES), f32),
            pltpu.VMEM((8, basis), f32),
            pltpu.VMEM((local, 2 * LANES), bf16),
            pltpu.VMEM((basis // SB, SB, 2 * LANES), f32),
            pltpu.VMEM((NCH, 2, 2, 64) + tile, f32),
            pltpu.VMEM((NCH, 2, 64) + tile, f32),
            pltpu.VMEM((NCH, 2, 32) + tile, f32),
            pltpu.VMEM((NCH, 2, 16) + tile, f32),
            pltpu.VMEM((NCH, 2, 3, 4) + tile, f32),
            pltpu.VMEM((NCH, ZS) + tile, f32),
            pltpu.VMEM((NCH, ZS - 1) + tile, f32),
            dma((13,)),
            dma((NCH,)), dma((NCH,)),
            dma((NCH, 2)), dma((NCH, 2)),
            dma((NCH, 2)), dma((NCH, 2)),
            dma((NCH, 2, 3)), dma((NCH, 2, 3)),
            dma((NCH, ZS - 1)), dma((NCH, ZS - 1)),
        ],
        compiler_params=pltpu.CompilerParams(
            collective_id=0, has_side_effects=True, vmem_limit_bytes=60 * 1024 * 1024),
        name="density",
    )(gamma, c_vir, c_occ, pair_list.T, shell_order)
    return summed.T.astype(bf16)


def solution(mesh):
    return jax.shard_map(
        shards,
        mesh=mesh,
        in_specs=(P("pair", "ao", None), P(), P(), P(), P()),
        out_specs=P("ao", "pair"),
        check_vma=False,
    )
```

```python
import jax
import jax.numpy as jnp
from jax import lax
from jax.experimental import pallas as pl
from jax.experimental.pallas import tpu as pltpu
from jax.sharding import PartitionSpec as P

MESH = pl.DeviceIdType.MESH
SB = 8
XS, YS, ZS = 4, 4, 8
NCH = 4
LANES = 128
UPFRONT = True
DIRECT = (3,)
ORDER = list(zip("lambwdvambwdvamebwdvamebwdveeffffgggghhhhiiii", (0, 0, 0, 0, 0, 0, 0, 1, 1, 1, 1, 1, 1, 2, 2, 0, 2, 2, 2, 2, 3, 3, 1, 3, 3, 3, 3, 2, 3, 0, 1, 2, 3, 0, 1, 2, 3, 0, 1, 2, 3, 0, 1, 2, 3)))


def kernel(gamma, c_vir, c_occ, pairs, shells, out, g, cv, co, pair_s, shell_s,
           lw, rw, half, block, s_buf, r_d, r_1, r_2, r_3, c_buf, r_z,
           in_sem, send, recv):
    local, vir = g.shape
    basis = cv.shape[0]
    pair = lax.axis_index("pair")
    xlo = lax.axis_index("ao")
    core = lax.rem(pair, 2)
    y = lax.rem(lax.div(pair, 2), YS)
    z = lax.rem(lax.div(pair, 2 * YS), ZS)
    xhi = lax.div(pair, 2 * YS * ZS)
    yhi, ylo = lax.div(y, 2), lax.rem(y, 2)

    def device(xh, xl, yy, zz, cc):
        return (((xh * ZS + zz) * YS + yy) * 2 + cc, xl)

    def relative(hi, lo, a, b, c):
        own = lax.rem(hi + lo * (1 - c), 2)
        low = lax.rem(lo + b, 2)
        return lax.rem(own + a + low * (1 - c), 2), low

    def x_peer(a, b):
        hi, lo = relative(xhi, xlo, a, b, core)
        return device(hi, lo, y, z, core)

    def y_peer(a, b):
        hi, lo = relative(yhi, ylo, a, b, core)
        return device(xhi, xlo, hi * 2 + lo, z, core)

    def z_peer(dz):
        return device(xhi, xlo, y, lax.rem(z + dz, ZS), core)

    twin = device(xhi, xlo, y, z, 1 - core)
    x_first = device(lax.rem(xhi + core, 2), 1 - xlo, y, z, core)
    y_first = device(xhi, xlo, lax.rem(yhi + core, 2) * 2 + (1 - ylo), z, core)
    x_second = x_peer(0, 1)
    y_second = y_peer(0, 1)

    own_half = xlo * (basis // 2)
    other_half = (1 - xlo) * (basis // 2)

    def row_starts(j):
        return (pl.multiple_of(own_half + j * LANES, LANES), pl.multiple_of(other_half + j * LANES, LANES))

    mid = local // 2

    def load(src, dst, k):
        copy = pltpu.make_async_copy(src, dst, in_sem.at[k])
        copy.start()
        return copy

    def load_rows(j, k):
        for start in row_starts(j):
            load(c_vir.at[pl.ds(start, LANES)], cv.at[pl.ds(start, LANES)], k)

    def wait_rows(chunks, k):
        rows = cv.at[pl.ds(0, chunks * 2 * LANES)]
        pltpu.make_async_copy(rows, rows, in_sem.at[k]).wait()

    load_shells = load(shells, shell_s, 0)
    load_pairs = load(pairs, pair_s, 1)
    load_occ = load(c_occ, co, 2)
    load_rows(0, 3)
    load_gamma = [load(gamma.at[0, pl.ds(t * mid, mid)], g.at[pl.ds(t * mid, mid)], 4 + t) for t in range(2)]
    if UPFRONT:
        for k in range(1, NCH):
            load_rows(k, 6)

    barrier = pltpu.get_barrier_semaphore()
    peers = [twin]
    peers += [x_peer(a, b) for a, b in ((0, 1), (1, 0), (1, 1))]
    peers += [y_peer(a, b) for a, b in ((0, 1), (1, 0), (1, 1))]
    peers += [z_peer(dz) for dz in range(1, ZS)]
    for peer in peers:
        pl.semaphore_signal(barrier, inc=1, device_id=peer, device_id_type=MESH)

    load_shells.wait()
    bits = [(a, b) for a in range(2) for b in range(2)]
    z_part = [lax.rem(z + dz, ZS) * (2 * YS) for dz in range(ZS)]
    x_part, x_turn, y_part = {}, {}, {}
    for d in range(2):
        cc = lax.rem(core + d, 2)
        for e in range(2):
            x_part[d, e] = lax.rem(xhi + e, 2) * (2 * YS * ZS) + cc
            x_turn[d, e] = lax.rem(e + 1 - cc, 2)
        for a, b in bits:
            hi, lo = relative(yhi, ylo, a, b, cc)
            y_part[d, a, b] = (hi * 2 + lo) * 2

    def weights():
        load_pairs.wait()
        load_occ.wait()
        left = pair_s[0, pair]
        right = pair_s[1, pair]
        occ = co.shape[1]
        pick = jnp.where(lax.broadcasted_iota(jnp.int32, (occ, LANES), 0) == left, 1.0, 0.0).astype(jnp.bfloat16)
        lw[...] = jnp.dot(co[...], pick, preferred_element_type=jnp.float32).reshape(lw.shape)
        pick = jnp.where(lax.broadcasted_iota(jnp.int32, (16, occ), 1) == right, 1.0, 0.0).astype(jnp.bfloat16)
        rw[...] = lax.dot_general(pick, co[...], (((1,), (1,)), ((), ())), preferred_element_type=jnp.float32)[:8]

    def compute_half(j, t):
        rhs = jnp.concatenate([cv[pl.ds(start, LANES), :] for start in row_starts(j)], axis=0)
        half[pl.ds(t * mid, mid), :] = lax.dot_general(
            g[pl.ds(t * mid, mid), :], rhs, (((1,), (1,)), ((), ())), preferred_element_type=jnp.float32
        ).astype(jnp.bfloat16)

    def compute_block(j):
        column = pl.multiple_of(xlo * local, LANES)
        tall = basis // 2
        for t in range(2):
            block[pl.ds(t * tall // SB, tall // SB)] = jnp.dot(
                cv[pl.ds(t * tall, tall), pl.ds(column, local)], half[...], preferred_element_type=jnp.float32
            ).reshape(tall // SB, SB, 2 * LANES)

    def remote(src, dst, kind, j, peer):
        return pltpu.make_async_remote_copy(
            src_ref=src, dst_ref=dst, send_sem=send.at[kind], recv_sem=recv.at[kind, j], device_id=peer,
            device_id_type=MESH)

    def wait_all(ref, semaphore):
        pltpu.make_async_copy(ref, ref, semaphore).wait()

    def send_d(j):
        remote(s_buf.at[j, 1], r_d.at[j], 0, j, twin).start()

    def send_1(j, part):
        remote(s_buf.at[j, 0, part, pl.ds(32, 32)], r_1.at[j, part], 1, j, (x_first, y_first)[part]).start()

    def send_2(j, part):
        remote(s_buf.at[j, 0, part, pl.ds(16, 16)], r_2.at[j, part], 2, j, (x_second, y_second)[part]).start()

    def send_a(j, part, t):
        a, b = bits[t]
        kind, into = (2, r_2.at[j, part]) if t == 1 else (1, r_1.at[j, part, pl.ds((t - 2) * 16, 16)])
        remote(s_buf.at[j, 0, part, pl.ds(t * 16, 16)], into, kind, j, (x_peer if part == 0 else y_peer)(a, b)).start()

    def send_3(j, part, t):
        a, b = bits[t]
        remote(s_buf.at[j, 0, part, pl.ds(t * 4, 4)], r_3.at[j, part, t - 1], 3, j,
               (y_peer if part == 0 else x_peer)(a, b)).start()

    def send_z(j, dz):
        remote(c_buf.at[j, dz], r_z.at[j, dz - 1], 4, j, z_peer(dz)).start()

    def weigh(j, d):
        right = [rw[:, pl.ds(start, LANES)] for start in row_starts(j)]
        for part in range(2):
            for e in range(2):
                for v in range(4):
                    xy = x_part[d, e] + y_part[(d,) + bits[v]]
                    if part == 0:
                        own, other = e * 32 + v * 4, x_turn[d, e] * 32 + 16 + v * 4
                    else:
                        own, other = v * 16 + e * 8, x_turn[d, e] * 8 + v * 16 + 4
                    for w in range(4):
                        shell = shell_s[xy + z_part[part * 4 + w]]
                        left = lw[shell]
                        s_buf[j, d, part, own + w] = block[shell, :, 0:LANES] * right[0] * left
                        s_buf[j, d, part, other + w] = block[shell, :, LANES : 2 * LANES] * right[1] * left

    def stage_l(j):
        weights()
        wait_rows(1, 3)
        load_gamma[0].wait()
        if not UPFRONT:
            for k in range(1, NCH):
                load_rows(k, 6)

    def stage_a(j):
        compute_half(j, 0)

    def stage_m(j):
        if j == 0:
            load_gamma[1].wait()
        compute_half(j, 1)

    def stage_b(j):
        if j == 0:
            wait_rows(NCH - 1, 6)
        compute_block(j)

    def stage_w(j):
        weigh(j, 1)

    def stage_v(j):
        weigh(j, 0)

    def stage_d(j):
        if j == 0:
            pl.semaphore_wait(barrier, len(peers))
        send_d(j)

    def stage_e(j):
        wait_all(r_d.at[j], recv.at[0, j])
        direct = j in DIRECT
        first = 16 if direct else 32
        for part in range(2):
            rest = pl.ds(first, 64 - first)
            s_buf[j, 0, part, rest] = s_buf[j, 0, part, rest] + r_d[j, part, rest]
            if direct:
                for t in (3, 2, 1):
                    send_a(j, part, t)
            else:
                send_1(j, part)
        for part in range(2):
            kept = pl.ds(0, first)
            s_buf[j, 0, part, kept] = s_buf[j, 0, part, kept] + r_d[j, part, kept]

    def stage_f(j):
        if j in DIRECT:
            return
        wait_all(r_1.at[j], recv.at[1, j])
        for part in range(2):
            s_buf[j, 0, part, pl.ds(16, 16)] = s_buf[j, 0, part, pl.ds(16, 16)] + r_1[j, part, pl.ds(0, 16)]
            send_2(j, part)
        for part in range(2):
            s_buf[j, 0, part, pl.ds(0, 16)] = s_buf[j, 0, part, pl.ds(0, 16)] + r_1[j, part, pl.ds(16, 16)]

    def stage_g(j):
        if j in DIRECT:
            wait_all(r_1.at[j], recv.at[1, j])
        wait_all(r_2.at[j], recv.at[2, j])
        for part in range(2):
            total = s_buf[j, 0, part, pl.ds(0, 16)] + r_2[j, part]
            if j in DIRECT:
                total = total + r_1[j, part, pl.ds(0, 16)] + r_1[j, part, pl.ds(16, 16)]
            s_buf[j, 0, part, pl.ds(0, 16)] = total
            for t in (3, 2, 1):
                send_3(j, part, t)

    def stage_h(j):
        wait_all(r_3.at[j], recv.at[3, j])
        for part in range(2):
            total = s_buf[j, 0, part, pl.ds(0, 4)]
            for t in range(3):
                total = total + r_3[j, part, t]
            c_buf[j, pl.ds(part * 4, 4)] = total
        for dz in (4, 3, 5, 2, 6, 1, 7):
            send_z(j, dz)

    def stage_i(j):
        wait_all(r_z.at[j], recv.at[4, j])
        total = c_buf[j, 0]
        for dz in range(1, ZS):
            total = total + r_z[j, dz - 1]
        out[:, j * LANES : (j + 1) * LANES] = total

    stages = dict(l=stage_l, a=stage_a, m=stage_m, b=stage_b, w=stage_w, v=stage_v, d=stage_d,
                  e=stage_e, f=stage_f, g=stage_g, h=stage_h, i=stage_i)
    for name, j in ORDER:
        stages[name](j)
    for kind, ref in enumerate((r_d, r_1, r_2, r_3, r_z)):
        wait_all(ref, send.at[kind])


def shards(gamma, c_vir, c_occ, pair_list, shell_order):
    local, vir = gamma.shape[1:]
    basis = c_vir.shape[0]
    f32, bf16 = jnp.float32, jnp.bfloat16
    dma = pltpu.SemaphoreType.DMA
    tile = (SB, LANES)
    summed = pl.pallas_call(
        kernel,
        out_shape=jax.ShapeDtypeStruct((SB, basis // 2), f32),
        in_specs=[pl.BlockSpec(memory_space=pl.ANY)] * 5,
        out_specs=pl.BlockSpec(memory_space=pltpu.VMEM),
        scratch_shapes=[
            pltpu.VMEM((local, vir), bf16),
            pltpu.VMEM((basis, vir), bf16),
            pltpu.VMEM(c_occ.shape, bf16),
            pltpu.SMEM((2, pair_list.shape[0]), jnp.int32),
            pltpu.SMEM(shell_order.shape, jnp.int32),
            pltpu.VMEM((basis // SB, SB, LANES), f32),
            pltpu.VMEM((8, basis), f32),
            pltpu.VMEM((local, 2 * LANES), bf16),
            pltpu.VMEM((basis // SB, SB, 2 * LANES), f32),
            pltpu.VMEM((NCH, 2, 2, 64) + tile, f32),
            pltpu.VMEM((NCH, 2, 64) + tile, f32),
            pltpu.VMEM((NCH, 2, 32) + tile, f32),
            pltpu.VMEM((NCH, 2, 16) + tile, f32),
            pltpu.VMEM((NCH, 2, 3, 4) + tile, f32),
            pltpu.VMEM((NCH, ZS) + tile, f32),
            pltpu.VMEM((NCH, ZS - 1) + tile, f32),
            dma((7,)),
            dma((5,)),
            dma((5, NCH)),
        ],
        compiler_params=pltpu.CompilerParams(
            collective_id=0, has_side_effects=True, vmem_limit_bytes=60 * 1024 * 1024),
        name="density",
    )(gamma, c_vir, c_occ, pair_list.T, shell_order)
    return summed.T.astype(bf16)


def solution(mesh):
    return jax.shard_map(
        shards,
        mesh=mesh,
        in_specs=(P("pair", "ao", None), P(), P(), P(), P()),
        out_specs=P("ao", "pair"),
        check_vma=False,
    )
```

```python
import jax
import jax.numpy as jnp
from jax import lax
from jax.experimental import pallas as pl
from jax.experimental.pallas import tpu as pltpu
from jax.sharding import PartitionSpec as P

MESH = pl.DeviceIdType.MESH
SB = 8
XS, YS, ZS = 4, 4, 8
NCH = 4
LANES = 128
DIRECT = (3,)
ORDER = list(zip("lambwdvambwdvamebwdvamebwdveefffgggghhhhiiii", (0, 0, 0, 0, 0, 0, 0, 1, 1, 1, 1, 1, 1, 2, 2, 0, 2, 2, 2, 2, 3, 3, 1, 3, 3, 3, 3, 2, 3, 0, 1, 2, 0, 1, 3, 2, 0, 1, 3, 2, 0, 1, 3, 2)))


def kernel(gamma, c_vir, c_occ, pairs, shells, out, g, cv, co, pair_s, shell_s,
           lw, rw, half, block, s_buf, r_d, r_1, r_2, r_3, c_buf, r_z,
           in_sem, send, recv):
    local, vir = g.shape
    basis = cv.shape[0]
    pair = lax.axis_index("pair")
    xlo = lax.axis_index("ao")
    core = lax.rem(pair, 2)
    y = lax.rem(lax.div(pair, 2), YS)
    z = lax.rem(lax.div(pair, 2 * YS), ZS)
    xhi = lax.div(pair, 2 * YS * ZS)
    yhi, ylo = lax.div(y, 2), lax.rem(y, 2)

    def device(xh, xl, yy, zz, cc):
        return (((xh * ZS + zz) * YS + yy) * 2 + cc, xl)

    def relative(hi, lo, a, b, c):
        own = lax.rem(hi + lo * (1 - c), 2)
        low = lax.rem(lo + b, 2)
        return lax.rem(own + a + low * (1 - c), 2), low

    def x_peer(a, b):
        hi, lo = relative(xhi, xlo, a, b, core)
        return device(hi, lo, y, z, core)

    def y_peer(a, b):
        hi, lo = relative(yhi, ylo, a, b, core)
        return device(xhi, xlo, hi * 2 + lo, z, core)

    def z_peer(dz):
        return device(xhi, xlo, y, lax.rem(z + dz, ZS), core)

    twin = device(xhi, xlo, y, z, 1 - core)
    x_first = device(lax.rem(xhi + core, 2), 1 - xlo, y, z, core)
    y_first = device(xhi, xlo, lax.rem(yhi + core, 2) * 2 + (1 - ylo), z, core)
    x_second = x_peer(0, 1)
    y_second = y_peer(0, 1)

    own_half = xlo * (basis // 2)
    other_half = (1 - xlo) * (basis // 2)

    def row_starts(j):
        return (pl.multiple_of(own_half + j * LANES, LANES), pl.multiple_of(other_half + j * LANES, LANES))

    mid = local // 2

    def load(src, dst, k):
        copy = pltpu.make_async_copy(src, dst, in_sem.at[k])
        copy.start()
        return copy

    def load_rows(j, k):
        for start in row_starts(j):
            load(c_vir.at[pl.ds(start, LANES)], cv.at[pl.ds(start, LANES)], k)

    def wait_rows(chunks, k):
        rows = cv.at[pl.ds(0, chunks * 2 * LANES)]
        pltpu.make_async_copy(rows, rows, in_sem.at[k]).wait()

    load_shells = load(shells, shell_s, 0)
    load_pairs = load(pairs, pair_s, 1)
    load_occ = load(c_occ, co, 2)
    load_rows(0, 3)
    load_gamma = [load(gamma.at[0, pl.ds(t * mid, mid)], g.at[pl.ds(t * mid, mid)], 4 + t) for t in range(2)]
    for k in range(1, NCH):
        load_rows(k, 6)

    barrier = pltpu.get_barrier_semaphore()
    peers = [twin]
    peers += [x_peer(a, b) for a, b in ((0, 1), (1, 0), (1, 1))]
    peers += [y_peer(a, b) for a, b in ((0, 1), (1, 0), (1, 1))]
    peers += [z_peer(dz) for dz in range(1, ZS)]
    for peer in peers:
        pl.semaphore_signal(barrier, inc=1, device_id=peer, device_id_type=MESH)

    load_shells.wait()
    bits = [(a, b) for a in range(2) for b in range(2)]
    z_part = [lax.rem(z + dz, ZS) * (2 * YS) for dz in range(ZS)]
    x_part, x_turn, y_part = {}, {}, {}
    for d in range(2):
        cc = lax.rem(core + d, 2)
        for e in range(2):
            x_part[d, e] = lax.rem(xhi + e, 2) * (2 * YS * ZS) + cc
            x_turn[d, e] = lax.rem(e + 1 - cc, 2)
        for a, b in bits:
            hi, lo = relative(yhi, ylo, a, b, cc)
            y_part[d, a, b] = (hi * 2 + lo) * 2

    def weights():
        load_pairs.wait()
        load_occ.wait()
        left = pair_s[0, pair]
        right = pair_s[1, pair]
        occ = co.shape[1]
        pick = jnp.where(lax.broadcasted_iota(jnp.int32, (occ, LANES), 0) == left, 1.0, 0.0).astype(jnp.bfloat16)
        lw[...] = jnp.dot(co[...], pick, preferred_element_type=jnp.float32).reshape(lw.shape)
        pick = jnp.where(lax.broadcasted_iota(jnp.int32, (16, occ), 1) == right, 1.0, 0.0).astype(jnp.bfloat16)
        rw[...] = lax.dot_general(pick, co[...], (((1,), (1,)), ((), ())), preferred_element_type=jnp.float32)[:8]

    def compute_half(j, t):
        rhs = jnp.concatenate([cv[pl.ds(start, LANES), :] for start in row_starts(j)], axis=0)
        half[pl.ds(t * mid, mid), :] = lax.dot_general(
            g[pl.ds(t * mid, mid), :], rhs, (((1,), (1,)), ((), ())), preferred_element_type=jnp.float32
        ).astype(jnp.bfloat16)

    def compute_block(j):
        column = pl.multiple_of(xlo * local, LANES)
        tall = basis // 2
        for t in range(2):
            block[pl.ds(t * tall // SB, tall // SB)] = jnp.dot(
                cv[pl.ds(t * tall, tall), pl.ds(column, local)], half[...], preferred_element_type=jnp.float32
            ).reshape(tall // SB, SB, 2 * LANES)

    def remote(src, dst, kind, j, peer):
        return pltpu.make_async_remote_copy(
            src_ref=src, dst_ref=dst, send_sem=send.at[kind], recv_sem=recv.at[kind, j], device_id=peer,
            device_id_type=MESH)

    def wait_all(ref, semaphore):
        pltpu.make_async_copy(ref, ref, semaphore).wait()

    def send_d(j):
        remote(s_buf.at[j, 1], r_d.at[j], 0, j, twin).start()

    def send_1(j, part):
        remote(s_buf.at[j, 0, part, pl.ds(32, 32)], r_1.at[j, part], 1, j, (x_first, y_first)[part]).start()

    def send_2(j, part):
        remote(s_buf.at[j, 0, part, pl.ds(16, 16)], r_2.at[j, part], 2, j, (x_second, y_second)[part]).start()

    def send_a(j, part, t):
        a, b = bits[t]
        kind, into = (2, r_2.at[j, part]) if t == 1 else (1, r_1.at[j, part, pl.ds((t - 2) * 16, 16)])
        remote(s_buf.at[j, 0, part, pl.ds(t * 16, 16)], into, kind, j, (x_peer if part == 0 else y_peer)(a, b)).start()

    def send_3(j, part, t):
        a, b = bits[t]
        remote(s_buf.at[j, 0, part, pl.ds(t * 4, 4)], r_3.at[j, part, t - 1], 3, j,
               (y_peer if part == 0 else x_peer)(a, b)).start()

    def send_z(j, dz):
        remote(c_buf.at[j, dz], r_z.at[j, dz - 1], 4, j, z_peer(dz)).start()

    def weigh(j, d):
        right = [rw[:, pl.ds(start, LANES)] for start in row_starts(j)]
        for part in range(2):
            for e in range(2):
                for v in range(4):
                    xy = x_part[d, e] + y_part[(d,) + bits[v]]
                    if part == 0:
                        own, other = e * 32 + v * 4, x_turn[d, e] * 32 + 16 + v * 4
                    else:
                        own, other = v * 16 + e * 8, x_turn[d, e] * 8 + v * 16 + 4
                    for w in range(4):
                        shell = shell_s[xy + z_part[part * 4 + w]]
                        left = lw[shell]
                        s_buf[j, d, part, own + w] = block[shell, :, 0:LANES] * right[0] * left
                        s_buf[j, d, part, other + w] = block[shell, :, LANES : 2 * LANES] * right[1] * left

    def stage_l(j):
        weights()
        wait_rows(1, 3)
        load_gamma[0].wait()

    def stage_a(j):
        compute_half(j, 0)

    def stage_m(j):
        if j == 0:
            load_gamma[1].wait()
        compute_half(j, 1)

    def stage_b(j):
        if j == 0:
            wait_rows(NCH - 1, 6)
        compute_block(j)

    def stage_w(j):
        weigh(j, 1)

    def stage_v(j):
        weigh(j, 0)

    def stage_d(j):
        if j == 0:
            pl.semaphore_wait(barrier, len(peers))
        send_d(j)

    def stage_e(j):
        wait_all(r_d.at[j], recv.at[0, j])
        direct = j in DIRECT
        first = 16 if direct else 32
        for part in range(2):
            rest = pl.ds(first, 64 - first)
            s_buf[j, 0, part, rest] = s_buf[j, 0, part, rest] + r_d[j, part, rest]
            if direct:
                for t in (2, 1, 3):
                    send_a(j, part, t)
            else:
                send_1(j, part)
        for part in range(2):
            kept = pl.ds(0, first)
            s_buf[j, 0, part, kept] = s_buf[j, 0, part, kept] + r_d[j, part, kept]

    def stage_f(j):
        if j in DIRECT:
            return
        wait_all(r_1.at[j], recv.at[1, j])
        for part in range(2):
            s_buf[j, 0, part, pl.ds(16, 16)] = s_buf[j, 0, part, pl.ds(16, 16)] + r_1[j, part, pl.ds(0, 16)]
            send_2(j, part)
        for part in range(2):
            s_buf[j, 0, part, pl.ds(0, 16)] = s_buf[j, 0, part, pl.ds(0, 16)] + r_1[j, part, pl.ds(16, 16)]

    def stage_g(j):
        if j in DIRECT:
            wait_all(r_1.at[j], recv.at[1, j])
        wait_all(r_2.at[j], recv.at[2, j])
        for part in range(2):
            total = s_buf[j, 0, part, pl.ds(0, 16)] + r_2[j, part]
            if j in DIRECT:
                total = total + r_1[j, part, pl.ds(0, 16)] + r_1[j, part, pl.ds(16, 16)]
            s_buf[j, 0, part, pl.ds(0, 16)] = total
            for t in (2, 1, 3):
                send_3(j, part, t)

    def stage_h(j):
        wait_all(r_3.at[j], recv.at[3, j])
        for part in range(2):
            total = s_buf[j, 0, part, pl.ds(0, 4)]
            for t in range(3):
                total = total + r_3[j, part, t]
            c_buf[j, pl.ds(part * 4, 4)] = total
        for dz in (4, 3, 5, 2, 6, 1, 7):
            send_z(j, dz)

    def stage_i(j):
        wait_all(r_z.at[j], recv.at[4, j])
        total = c_buf[j, 0]
        for dz in range(1, ZS):
            total = total + r_z[j, dz - 1]
        out[:, j * LANES : (j + 1) * LANES] = total

    stages = dict(l=stage_l, a=stage_a, m=stage_m, b=stage_b, w=stage_w, v=stage_v, d=stage_d,
                  e=stage_e, f=stage_f, g=stage_g, h=stage_h, i=stage_i)
    for name, j in ORDER:
        stages[name](j)
    for kind, ref in enumerate((r_d, r_1, r_2, r_3, r_z)):
        wait_all(ref, send.at[kind])


def shards(gamma, c_vir, c_occ, pair_list, shell_order):
    local, vir = gamma.shape[1:]
    basis = c_vir.shape[0]
    f32, bf16 = jnp.float32, jnp.bfloat16
    dma = pltpu.SemaphoreType.DMA
    tile = (SB, LANES)
    summed = pl.pallas_call(
        kernel,
        out_shape=jax.ShapeDtypeStruct((SB, basis // 2), f32),
        in_specs=[pl.BlockSpec(memory_space=pl.ANY)] * 5,
        out_specs=pl.BlockSpec(memory_space=pltpu.VMEM),
        scratch_shapes=[
            pltpu.VMEM((local, vir), bf16),
            pltpu.VMEM((basis, vir), bf16),
            pltpu.VMEM(c_occ.shape, bf16),
            pltpu.SMEM((2, pair_list.shape[0]), jnp.int32),
            pltpu.SMEM(shell_order.shape, jnp.int32),
            pltpu.VMEM((basis // SB, SB, LANES), f32),
            pltpu.VMEM((8, basis), f32),
            pltpu.VMEM((local, 2 * LANES), bf16),
            pltpu.VMEM((basis // SB, SB, 2 * LANES), f32),
            pltpu.VMEM((NCH, 2, 2, 64) + tile, f32),
            pltpu.VMEM((NCH, 2, 64) + tile, f32),
            pltpu.VMEM((NCH, 2, 32) + tile, f32),
            pltpu.VMEM((NCH, 2, 16) + tile, f32),
            pltpu.VMEM((NCH, 2, 3, 4) + tile, f32),
            pltpu.VMEM((NCH, ZS) + tile, f32),
            pltpu.VMEM((NCH, ZS - 1) + tile, f32),
            dma((7,)),
            dma((5,)),
            dma((5, NCH)),
        ],
        compiler_params=pltpu.CompilerParams(
            collective_id=0, has_side_effects=True, vmem_limit_bytes=60 * 1024 * 1024),
        name="density",
    )(gamma, c_vir, c_occ, pair_list.T, shell_order)
    return summed.T.astype(bf16)


def solution(mesh):
    return jax.shard_map(
        shards,
        mesh=mesh,
        in_specs=(P("pair", "ao", None), P(), P(), P(), P()),
        out_specs=P("ao", "pair"),
        check_vma=False,
    )
```

```python
import jax
import jax.numpy as jnp
from jax import lax
from jax.experimental import pallas as pl
from jax.experimental.pallas import tpu as pltpu
from jax.sharding import PartitionSpec as P

MESH = pl.DeviceIdType.MESH
SB = 8
XS, YS, ZS = 4, 4, 8
NCH = 4
LANES = 128
DIRECT = (3,)
ORDER = list(zip("lambwdvambwdvamebwdvamebwdevefffgggghhhhi", (0, 0, 0, 0, 0, 0, 0, 1, 1, 1, 1, 1, 1, 2, 2, 0, 2, 2, 2, 2, 3, 3, 1, 3, 3, 3, 2, 3, 3, 0, 1, 2, 0, 1, 3, 2, 0, 1, 3, 2, 0)))


def kernel(gamma, c_vir, c_occ, pairs, shells, out, g, cv, co, pair_s, shell_s,
           lw, rw, half, block, s_buf, r_d, r_1, r_2, r_3, c_buf, r_z,
           in_sem, send, recv):
    local, vir = g.shape
    basis = cv.shape[0]
    pair = lax.axis_index("pair")
    xlo = lax.axis_index("ao")
    core = lax.rem(pair, 2)
    y = lax.rem(lax.div(pair, 2), YS)
    z = lax.rem(lax.div(pair, 2 * YS), ZS)
    xhi = lax.div(pair, 2 * YS * ZS)
    yhi, ylo = lax.div(y, 2), lax.rem(y, 2)

    def device(xh, xl, yy, zz, cc):
        return (((xh * ZS + zz) * YS + yy) * 2 + cc, xl)

    def relative(hi, lo, a, b, c):
        own = lax.rem(hi + lo * (1 - c), 2)
        low = lax.rem(lo + b, 2)
        return lax.rem(own + a + low * (1 - c), 2), low

    def x_peer(a, b):
        hi, lo = relative(xhi, xlo, a, b, core)
        return device(hi, lo, y, z, core)

    def y_peer(a, b):
        hi, lo = relative(yhi, ylo, a, b, core)
        return device(xhi, xlo, hi * 2 + lo, z, core)

    def z_peer(dz):
        return device(xhi, xlo, y, lax.rem(z + dz, ZS), core)

    twin = device(xhi, xlo, y, z, 1 - core)
    x_first = device(lax.rem(xhi + core, 2), 1 - xlo, y, z, core)
    y_first = device(xhi, xlo, lax.rem(yhi + core, 2) * 2 + (1 - ylo), z, core)
    x_second = x_peer(0, 1)
    y_second = y_peer(0, 1)

    own_half = xlo * (basis // 2)
    other_half = (1 - xlo) * (basis // 2)

    def row_starts(j):
        return (pl.multiple_of(own_half + j * LANES, LANES), pl.multiple_of(other_half + j * LANES, LANES))

    mid = local // 2

    def load(src, dst, k):
        copy = pltpu.make_async_copy(src, dst, in_sem.at[k])
        copy.start()
        return copy

    def load_rows(j, k):
        for start in row_starts(j):
            load(c_vir.at[pl.ds(start, LANES)], cv.at[pl.ds(start, LANES)], k)

    def wait_rows(chunks, k):
        rows = cv.at[pl.ds(0, chunks * 2 * LANES)]
        pltpu.make_async_copy(rows, rows, in_sem.at[k]).wait()

    load_shells = load(shells, shell_s, 0)
    load_pairs = load(pairs, pair_s, 1)
    load_occ = load(c_occ, co, 2)
    load_rows(0, 3)
    load_gamma = [load(gamma.at[0, pl.ds(t * mid, mid)], g.at[pl.ds(t * mid, mid)], 4 + t) for t in range(2)]
    for k in range(1, NCH):
        load_rows(k, 6)

    barrier = pltpu.get_barrier_semaphore()
    peers = [twin]
    peers += [x_peer(a, b) for a, b in ((0, 1), (1, 0), (1, 1))]
    peers += [y_peer(a, b) for a, b in ((0, 1), (1, 0), (1, 1))]
    peers += [z_peer(dz) for dz in range(1, ZS)]
    for peer in peers:
        pl.semaphore_signal(barrier, inc=1, device_id=peer, device_id_type=MESH)

    load_shells.wait()
    bits = [(a, b) for a in range(2) for b in range(2)]
    z_part = [lax.rem(z + dz, ZS) * (2 * YS) for dz in range(ZS)]
    x_part, x_turn, y_part = {}, {}, {}
    for d in range(2):
        cc = lax.rem(core + d, 2)
        for e in range(2):
            x_part[d, e] = lax.rem(xhi + e, 2) * (2 * YS * ZS) + cc
            x_turn[d, e] = lax.rem(e + 1 - cc, 2)
        for a, b in bits:
            hi, lo = relative(yhi, ylo, a, b, cc)
            y_part[d, a, b] = (hi * 2 + lo) * 2

    def weights():
        load_pairs.wait()
        load_occ.wait()
        left = pair_s[0, pair]
        right = pair_s[1, pair]
        occ = co.shape[1]
        pick = jnp.where(lax.broadcasted_iota(jnp.int32, (occ, LANES), 0) == left, 1.0, 0.0).astype(jnp.bfloat16)
        lw[...] = jnp.dot(co[...], pick, preferred_element_type=jnp.float32).reshape(lw.shape)
        pick = jnp.where(lax.broadcasted_iota(jnp.int32, (16, occ), 1) == right, 1.0, 0.0).astype(jnp.bfloat16)
        rw[...] = lax.dot_general(pick, co[...], (((1,), (1,)), ((), ())), preferred_element_type=jnp.float32)[:8]

    def compute_half(j, t):
        rhs = jnp.concatenate([cv[pl.ds(start, LANES), :] for start in row_starts(j)], axis=0)
        half[pl.ds(t * mid, mid), :] = lax.dot_general(
            g[pl.ds(t * mid, mid), :], rhs, (((1,), (1,)), ((), ())), preferred_element_type=jnp.float32
        ).astype(jnp.bfloat16)

    def compute_block(j):
        column = pl.multiple_of(xlo * local, LANES)
        tall = basis // 2
        for t in range(2):
            block[pl.ds(t * tall // SB, tall // SB)] = jnp.dot(
                cv[pl.ds(t * tall, tall), pl.ds(column, local)], half[...], preferred_element_type=jnp.float32
            ).reshape(tall // SB, SB, 2 * LANES)

    def remote(src, dst, kind, j, peer):
        return pltpu.make_async_remote_copy(
            src_ref=src, dst_ref=dst, send_sem=send.at[kind], recv_sem=recv.at[kind * NCH + (j if kind < 4 else 0)], device_id=peer,
            device_id_type=MESH)

    def wait_all(ref, semaphore):
        pltpu.make_async_copy(ref, ref, semaphore).wait()

    def send_d(j):
        remote(s_buf.at[j, 1], r_d.at[j], 0, j, twin).start()

    def send_1(j, part):
        remote(s_buf.at[j, 0, part, pl.ds(32, 32)], r_1.at[j, part], 1, j, (x_first, y_first)[part]).start()

    def send_2(j, part):
        remote(s_buf.at[j, 0, part, pl.ds(16, 16)], r_2.at[j, part], 2, j, (x_second, y_second)[part]).start()

    def send_a(j, part, t):
        a, b = bits[t]
        kind, into = (2, r_2.at[j, part]) if t == 1 else (1, r_1.at[j, part, pl.ds((t - 2) * 16, 16)])
        remote(s_buf.at[j, 0, part, pl.ds(t * 16, 16)], into, kind, j, (x_peer if part == 0 else y_peer)(a, b)).start()

    def send_3(j, part, t):
        a, b = bits[t]
        remote(s_buf.at[j, 0, part, pl.ds(t * 4, 4)], r_3.at[j, part, t - 1], 3, j,
               (y_peer if part == 0 else x_peer)(a, b)).start()

    def send_z(j, dz):
        remote(c_buf.at[j, dz], r_z.at[j, dz - 1], 4, j, z_peer(dz)).start()

    def weigh(j, d):
        right = [rw[:, pl.ds(start, LANES)] for start in row_starts(j)]
        for part in range(2):
            for e in range(2):
                for v in range(4):
                    xy = x_part[d, e] + y_part[(d,) + bits[v]]
                    if part == 0:
                        own, other = e * 32 + v * 4, x_turn[d, e] * 32 + 16 + v * 4
                    else:
                        own, other = v * 16 + e * 8, x_turn[d, e] * 8 + v * 16 + 4
                    for w in range(4):
                        shell = shell_s[xy + z_part[part * 4 + w]]
                        left = lw[shell]
                        s_buf[j, d, part, own + w] = block[shell, :, 0:LANES] * right[0] * left
                        s_buf[j, d, part, other + w] = block[shell, :, LANES : 2 * LANES] * right[1] * left

    def stage_l(j):
        weights()
        wait_rows(1, 3)
        load_gamma[0].wait()

    def stage_a(j):
        compute_half(j, 0)

    def stage_m(j):
        if j == 0:
            load_gamma[1].wait()
        compute_half(j, 1)

    def stage_b(j):
        if j == 0:
            wait_rows(NCH - 1, 6)
        compute_block(j)

    def stage_w(j):
        weigh(j, 1)

    def stage_v(j):
        weigh(j, 0)

    def stage_d(j):
        if j == 0:
            pl.semaphore_wait(barrier, len(peers))
        send_d(j)

    def stage_e(j):
        wait_all(r_d.at[j], recv.at[0 * NCH + j])
        direct = j in DIRECT
        first = 16 if direct else 32
        for part in range(2):
            rest = pl.ds(first, 64 - first)
            s_buf[j, 0, part, rest] = s_buf[j, 0, part, rest] + r_d[j, part, rest]
            if direct:
                for t in (2, 1, 3):
                    send_a(j, part, t)
            else:
                send_1(j, part)
        for part in range(2):
            kept = pl.ds(0, first)
            s_buf[j, 0, part, kept] = s_buf[j, 0, part, kept] + r_d[j, part, kept]

    def stage_f(j):
        if j in DIRECT:
            return
        wait_all(r_1.at[j], recv.at[1 * NCH + j])
        for part in range(2):
            s_buf[j, 0, part, pl.ds(16, 16)] = s_buf[j, 0, part, pl.ds(16, 16)] + r_1[j, part, pl.ds(0, 16)]
            send_2(j, part)
        for part in range(2):
            s_buf[j, 0, part, pl.ds(0, 16)] = s_buf[j, 0, part, pl.ds(0, 16)] + r_1[j, part, pl.ds(16, 16)]

    def stage_g(j):
        if j in DIRECT:
            wait_all(r_1.at[j], recv.at[1 * NCH + j])
        wait_all(r_2.at[j], recv.at[2 * NCH + j])
        for part in range(2):
            total = s_buf[j, 0, part, pl.ds(0, 16)] + r_2[j, part]
            if j in DIRECT:
                total = total + r_1[j, part, pl.ds(0, 16)] + r_1[j, part, pl.ds(16, 16)]
            s_buf[j, 0, part, pl.ds(0, 16)] = total
            for t in (2, 1, 3):
                send_3(j, part, t)

    def stage_h(j):
        wait_all(r_3.at[j], recv.at[3 * NCH + j])
        for part in range(2):
            total = s_buf[j, 0, part, pl.ds(0, 4)]
            for t in range(3):
                total = total + r_3[j, part, t]
            c_buf[j, pl.ds(part * 4, 4)] = total
        for dz in (4, 3, 5, 2, 6, 1, 7):
            send_z(j, dz)

    def stage_i(j):
        wait_all(r_z, recv.at[4 * NCH])
        for k in range(NCH):
            total = c_buf[k, 0]
            for dz in range(1, ZS):
                total = total + r_z[k, dz - 1]
            out[:, k * LANES : (k + 1) * LANES] = total

    stages = dict(l=stage_l, a=stage_a, m=stage_m, b=stage_b, w=stage_w, v=stage_v, d=stage_d,
                  e=stage_e, f=stage_f, g=stage_g, h=stage_h, i=stage_i)
    for name, j in ORDER:
        stages[name](j)
    for kind, ref in enumerate((r_d, r_1, r_2, r_3, r_z)):
        wait_all(ref, send.at[kind])


def shards(gamma, c_vir, c_occ, pair_list, shell_order):
    local, vir = gamma.shape[1:]
    basis = c_vir.shape[0]
    f32, bf16 = jnp.float32, jnp.bfloat16
    dma = pltpu.SemaphoreType.DMA
    tile = (SB, LANES)
    summed = pl.pallas_call(
        kernel,
        out_shape=jax.ShapeDtypeStruct((SB, basis // 2), f32),
        in_specs=[pl.BlockSpec(memory_space=pl.ANY)] * 5,
        out_specs=pl.BlockSpec(memory_space=pltpu.VMEM),
        scratch_shapes=[
            pltpu.VMEM((local, vir), bf16),
            pltpu.VMEM((basis, vir), bf16),
            pltpu.VMEM(c_occ.shape, bf16),
            pltpu.SMEM((2, pair_list.shape[0]), jnp.int32),
            pltpu.SMEM(shell_order.shape, jnp.int32),
            pltpu.VMEM((basis // SB, SB, LANES), f32),
            pltpu.VMEM((8, basis), f32),
            pltpu.VMEM((local, 2 * LANES), bf16),
            pltpu.VMEM((basis // SB, SB, 2 * LANES), f32),
            pltpu.VMEM((NCH, 2, 2, 64) + tile, f32),
            pltpu.VMEM((NCH, 2, 64) + tile, f32),
            pltpu.VMEM((NCH, 2, 32) + tile, f32),
            pltpu.VMEM((NCH, 2, 16) + tile, f32),
            pltpu.VMEM((NCH, 2, 3, 4) + tile, f32),
            pltpu.VMEM((NCH, ZS) + tile, f32),
            pltpu.VMEM((NCH, ZS - 1) + tile, f32),
            dma((7,)),
            dma((5,)),
            dma((4 * NCH + 1,)),
        ],
        compiler_params=pltpu.CompilerParams(
            collective_id=0, has_side_effects=True, vmem_limit_bytes=60 * 1024 * 1024),
        name="density",
    )(gamma, c_vir, c_occ, pair_list.T, shell_order)
    return summed.T.astype(bf16)


def solution(mesh):
    return jax.shard_map(
        shards,
        mesh=mesh,
        in_specs=(P("pair", "ao", None), P(), P(), P(), P()),
        out_specs=P("ao", "pair"),
        check_vma=False,
    )
```
